128 devices in a mesh: seq: 32 (over y, x, z_hi), grp: 4 (over z_lo, core).
Axes of the slice: x: 4, y: 4, z: 4 (z_hi: 2, z_lo: 2; z = z_hi * 2 + z_lo), core: 2. Of those that a mesh axis runs over, the one named last changes fastest.
Arguments:
- queries: bfloat16 [32768, 4096], P(('grp', 'seq')), parts along dimension 0, may hold values from -64 to 64
- keys: bfloat16 [32768, 1024], P(('grp', 'seq')), parts along dimension 0, may hold values from -64 to 64
- values: bfloat16 [32768, 1024], P(('grp', 'seq')), parts along dimension 0, may hold values from -6 to 6
- doc_lengths: int32 [24], P('grp'), parts along dimension 0, may hold values from 1 to 32, 64 in all
Outputs:
- attended: bfloat16 [32768, 4096], P(('grp', 'seq')), parts along dimension 0
The draws below stay inside these ranges and needn't reach their ends.
There are 4 independent parts, one for each index of `grp`. The reference program is written for one: setup_inputs(seed, part) draws one part's arguments, and reference() takes and returns one part's arrays. A program takes and returns all parts, laid end to end along the dimension named above; each array names one. Nothing has to cross between parts.
Inputs may be any that keep to these rules, and one draw needn't show every extreme that they name: `doc_lengths`: lengths of the documents in units of 128 tokens, summing to 64.
All inputs are finite; a program needn't handle non-finite values.
Results may differ from the reference program's by a relative error of at most 0.004.
Values may be sent and summed in bfloat16 or wider, within the bound.
A program may use at most 128 MiB of HBM per device.

```python
import math
import jax
import jax.numpy as jnp
import numpy as np
from jax import lax

HEADS = 32
KV_HEADS = 8
HEAD_DIM = 128
DOC_UNIT = 128
DOCS = 6
TOKENS = 8192
UNITS = 64


def drawn(key):
    base = jax.random.fold_in(key, 7)
    key_a, key_b = jax.random.split(base, 2)
    group_size = HEADS // KV_HEADS
    key_vectors = jax.random.normal(key_a, (TOKENS, KV_HEADS, HEAD_DIM), jnp.float32)
    query_vectors = jax.random.normal(key_b, (TOKENS, KV_HEADS, group_size, HEAD_DIM), jnp.float32)
    return (query_vectors.reshape(TOKENS, HEADS * HEAD_DIM), key_vectors.reshape(TOKENS, KV_HEADS * HEAD_DIM))


def draw_queries(key, part):
    return drawn(key)[0].astype(jnp.bfloat16)


def draw_keys(key, part):
    return drawn(key)[1].astype(jnp.bfloat16)


def shard_levels(own_key, extent, cuts, least, top_value):
    factor_of, own = 1.0, jax.random.fold_in(own_key, 6)
    for dim, shards_of in cuts:
        heights = jnp.exp(jax.random.uniform(jax.random.fold_in(own, dim), (shards_of,), jnp.float32, least / len(cuts), top_value / len(cuts)))
        factor_of = factor_of * jnp.repeat(heights, extent[dim] // shards_of).reshape([-1 if axis == dim else 1 for axis in range(len(extent))])
    return factor_of


def split_up(count, total, reach, skew):
    weights = [(1 << 20) // math.isqrt(grade ** skew) + 1 for grade in range(2, count + 1)]
    surplus, given = total - reach - (count - 1), [1] * (count - 1)
    while surplus > 0:
        free = [i for i in range(count - 1) if given[i] < reach]
        mass, left = sum([weights[i] for i in free]), surplus
        for i in free:
            more = min(reach - given[i], max(1, left * weights[i] // mass), surplus)
            given[i] = given[i] + more
            surplus = surplus - more
    return np.array([reach] + given)


def uneven(rng, amount, total, most, lean):
    if amount == 2:
        one = jax.random.randint(rng, (), max(1, total - most), min(most, total - 1) + 1)
        return jnp.stack([one, total - one])
    tallies = jnp.asarray(split_up(amount, total, most, lean), jnp.int32)
    pairs = (amount - 1) // 2
    giver, sink = tallies[1:1 + 2 * pairs:2], tallies[2:2 + 2 * pairs:2]
    slack = jnp.minimum(giver - 1, most - sink)
    passed = jax.random.randint(jax.random.fold_in(rng, 1), (pairs,), 0, 1 << 20) % (slack + 1)
    tallies = tallies.at[1:1 + 2 * pairs:2].set(giver - passed).at[2:2 + 2 * pairs:2].set(sink + passed)
    return tallies[jax.random.permutation(jax.random.fold_in(rng, 2), amount)]


def centred(stream_key, dims, width, reach, cuts=(), held_as=jnp.bfloat16):
    values = width * jax.random.normal(stream_key, dims, jnp.float32)
    if cuts:
        values = values * shard_levels(stream_key, dims, cuts, -0.22, 0.18)
    return jnp.clip(values, -reach, reach).astype(held_as)


def setup_inputs(seed: int = 0, part: int = 0) -> dict:
    key_list = jax.random.split(jax.random.key(seed), 5)
    own_keys = jax.random.split(jax.random.fold_in(key_list[4], part), 5)
    return {
        "queries": draw_queries(jax.random.fold_in(jax.random.fold_in(key_list[4], part), 71), part),
        "keys": draw_keys(jax.random.fold_in(jax.random.fold_in(key_list[4], part), 71), part),
        "values": centred(own_keys[2], (TOKENS, KV_HEADS * HEAD_DIM), 1.0, 6.0, ((0, 32),)),
        "doc_lengths": uneven(own_keys[3], DOCS, UNITS, UNITS // 2, 2).astype(jnp.int32),
    }


def reference(queries, keys, values, doc_lengths):
    group_size = HEADS // KV_HEADS
    scale = HEAD_DIM ** -0.5
    grouped = queries.reshape(TOKENS, KV_HEADS, group_size, HEAD_DIM).transpose(1, 0, 2, 3)
    key_heads = keys.reshape(TOKENS, KV_HEADS, HEAD_DIM).transpose(1, 0, 2)
    value_heads = values.reshape(TOKENS, KV_HEADS, HEAD_DIM).transpose(1, 0, 2)
    positions = jnp.arange(TOKENS, dtype=jnp.int32)
    lengths = (doc_lengths * DOC_UNIT).astype(jnp.int32)
    starts = (jnp.cumsum(lengths) - lengths).astype(jnp.int32)
    documents = jnp.sum((positions[:, None] >= starts[None, :]).astype(jnp.int32), axis=1)
    block_rows = math.gcd(TOKENS, 1024)
    pieces = []
    for first_row in range(0, TOKENS, block_rows):
        last_row = first_row + block_rows
        allowed = (positions[None, :last_row] <= positions[first_row:last_row, None]) & (
            documents[None, :last_row] == documents[first_row:last_row, None])

        def per_head(operands, allowed=allowed):
            query_head, key_head, value_head = operands
            scores = jnp.einsum("qgd,kd->gqk", query_head.astype(jnp.float32), key_head.astype(jnp.float32)) * scale
            scores = jnp.where(allowed[None], scores, -jnp.inf)
            weights = jnp.exp(scores - jnp.max(scores, axis=-1, keepdims=True))
            totals = jnp.sum(weights, axis=-1)
            rounded = lax.optimization_barrier(weights.astype(jnp.bfloat16)).astype(jnp.float32)
            mixed = jnp.einsum("gqk,kd->qgd", rounded, value_head.astype(jnp.float32))
            return mixed / jnp.transpose(totals)[:, :, None]

        outputs = lax.map(per_head, (grouped[:, first_row:last_row], key_heads[:, :last_row], value_heads[:, :last_row]))
        pieces.append(outputs.transpose(1, 0, 2, 3).reshape(block_rows, HEADS * HEAD_DIM))
    return jnp.concatenate(pieces, axis=0).astype(jnp.bfloat16)
```

```python
import functools

import jax
import jax.numpy as jnp
from jax import lax
from jax.experimental import pallas as pl
from jax.experimental.pallas import tpu as pltpu
from jax.sharding import PartitionSpec as P

DIM = 128
UNIT = 128
ROWS = 256
TOKENS = 8192
DOCS = 6
TILE = 1024
CHUNK = 512
UNITS = 4
VROWS = 136
SCALE = float(DIM**-0.5 * 1.4426950408889634)
FAR = float(2**21)
NEG = -1e30
MESH = pl.DeviceIdType.MESH


def kernel(
    lengths, q_hbm, k_hbm, v_hbm, out_hbm,
    qin, kbuf, vbuf, vt, kext, qfeat, qx, acc, s_scr, p_scr, obuf,
    q_send, q_recv, a_send, a_recv, f_send, f_recv, o_send, o_recv,
):
    me = lax.axis_index("seq")
    y, x, z = me // 8, (me // 2) % 4, me % 2
    xh, xl = x // 2, x % 2
    mine = 2 * y + xl
    x_mate = y * 8 + (3 - x) * 2 + z
    z_mate = y * 8 + x * 2 + 1 - z

    def device(j):
        return (j // 2) * 8 + (2 * xh + j % 2) * 2 + z

    def head(j):
        return 2 * (j // 2) + (j % 2 + xh) % 2

    def block(j, half, side):
        number = (j // 2) * 8 + (2 * half + j % 2) * 2 + side
        return pl.ds(pl.multiple_of(number * ROWS, ROWS), ROWS)

    def cols(start, size):
        return pl.ds(pl.multiple_of(start, DIM), size)

    def remote(src, dst, send, recv, to):
        return pltpu.make_async_remote_copy(
            src_ref=src, dst_ref=dst, send_sem=send, recv_sem=recv,
            device_id={"seq": to}, device_id_type=MESH,
        )

    def kv_in(which, j_from, j_to):
        hbm, buf = ((k_hbm, kbuf), (v_hbm, vbuf))[which]
        return (
            hbm.at[:, cols(head(j_to) * DIM, DIM)],
            buf.at[block(j_from, xh, z), :],
        )

    def q_in(ph, j_from, j_to):
        return (
            q_hbm.at[:, cols(head(j_to) * 4 * DIM + ph * 2 * DIM, 2 * DIM)],
            qin.at[ph, j_from],
        )

    def kv_copy(which, j_to):
        src, dst = kv_in(which, mine, j_to)
        return remote(src, dst, a_send.at[which, j_to], a_recv.at[which, mine], device(j_to))

    def q_copy(ph, j_to):
        src, dst = q_in(ph, mine, j_to)
        return remote(src, dst, q_send.at[ph, j_to], q_recv.at[ph, mine], device(j_to))

    def kv_arrived(which, j):
        src, dst = kv_in(which, j, mine)
        return remote(src, dst, a_send.at[which, j], a_recv.at[which, j], device(j))

    def q_arrived(ph, j):
        src, dst = q_in(ph, j, mine)
        return remote(src, dst, q_send.at[ph, j], q_recv.at[ph, j], device(j))

    def forward(kind, j, sending):
        buf = kbuf if kind in (0, 1, 4) else vbuf
        to = z_mate if kind in (0, 2, 5) else x_mate
        half, side = xh, z
        if sending:
            if kind == 4:
                side = 1 - z
            if kind == 5:
                half = 1 - xh
        else:
            if kind in (0, 2):
                side = 1 - z
            elif kind in (1, 3):
                half = 1 - xh
            else:
                half, side = 1 - xh, 1 - z
        rows = buf.at[block(j, half, side), :]
        return remote(rows, rows, f_send.at[kind, j], f_recv.at[kind, j], to)

    barrier = pltpu.get_barrier_semaphore()

    def greet(o, c):
        pl.semaphore_signal(
            barrier, inc=1, device_id={"seq": device((mine + o) % 8)}, device_id_type=MESH
        )
        return c

    own = []
    for which in range(2):
        src, dst = kv_in(which, mine, mine)
        own.append(pltpu.make_async_copy(src, dst, a_recv.at[which, mine]))
    for ph in range(2):
        src, dst = q_in(ph, mine, mine)
        own.append(pltpu.make_async_copy(src, dst, q_recv.at[ph, mine]))
    for copy in own:
        copy.start()
    lax.fori_loop(1, 8, greet, 0)
    pl.semaphore_signal(barrier, inc=1, device_id={"seq": x_mate}, device_id_type=MESH)
    pl.semaphore_signal(barrier, inc=1, device_id={"seq": z_mate}, device_id_type=MESH)
    pl.semaphore_wait(barrier, 9)

    def send_kv(o, c):
        for which in range(2):
            kv_copy(which, (mine + o) % 8).start()
        return c

    def send_q(ph):
        def go(o, c):
            q_copy(ph, (mine + o) % 8).start()
            return c

        lax.fori_loop(1, 8, go, 0)

    lax.fori_loop(1, 8, send_kv, 0)
    send_q(0)
    send_q(1)

    starts, total = [], jnp.int32(0)
    for d in range(DOCS):
        starts.append(total)
        total = total + lengths[d] * UNIT
    ends = starts[1:] + [total]

    lane = lax.broadcasted_iota(jnp.int32, (1, DIM), 1)
    low, high = jnp.zeros((1, DIM), jnp.int32), jnp.full((1, DIM), TOKENS, jnp.int32)
    for d in range(DOCS):
        low, high = jnp.where(lane == d, starts[d], low), jnp.where(lane == d, ends[d], high)

    def key_features(i, c):
        first = pl.multiple_of(i * ROWS, ROWS)
        token = first + lax.broadcasted_iota(jnp.int32, (ROWS, DIM), 0)
        inside = (token >= low) & (token < high)
        kext[pl.ds(first, ROWS), :] = jnp.where(inside, 0.0, -FAR).astype(jnp.bfloat16)
        return c

    feature = lax.broadcasted_iota(jnp.int32, (DIM, ROWS), 0)
    low_row, high_row = jnp.full((DIM, ROWS), TOKENS, jnp.int32), jnp.zeros((DIM, ROWS), jnp.int32)
    for d in range(DOCS):
        low_row = jnp.where(feature == d, starts[d], low_row)
        high_row = jnp.where(feature == d, ends[d], high_row)

    def query_features(j, c):
        first = ((j // 2) * 8 + (2 * xh + j % 2) * 2 + z) * ROWS
        token = first + lax.broadcasted_iota(jnp.int32, (DIM, ROWS), 1)
        inside = (token >= low_row) & (token < high_row)
        qfeat[j] = jnp.where(inside, 1.0, 0.0).astype(jnp.bfloat16)
        return c

    ones = lax.broadcasted_iota(jnp.int32, (VROWS - DIM, ROWS), 0) == 0
    ones = jnp.where(ones, 1.0, 0.0).astype(jnp.bfloat16)

    def hop1(r):
        for j in (2 * r, 2 * r + 1):
            kv_arrived(0, j).wait_recv()
            forward(0, j, True).start()
            forward(1, j, True).start()
            kv_arrived(1, j).wait_recv()
            forward(2, j, True).start()
            forward(3, j, True).start()

    def relay(r):
        for j in (2 * r, 2 * r + 1):
            forward(0, j, False).wait_recv()
            forward(4, j, True).start()
            forward(3, j, False).wait_recv()
            forward(5, j, True).start()

    hop1(0)
    hop1(1)
    lax.fori_loop(0, TOKENS // ROWS, key_features, 0)
    relay(0)
    hop1(2)
    lax.fori_loop(0, 8, query_features, 0)
    relay(1)
    hop1(3)

    def receive_row(r):
        for j in (2 * r, 2 * r + 1):
            for kind in (1, 2, 4, 5):
                forward(kind, j, False).wait_recv()

        def turn(i, c):
            rows = pl.ds(pl.multiple_of((8 * r + i) * ROWS, ROWS), ROWS)
            vt[:DIM, rows] = vbuf[rows, :].T
            vt[DIM:, rows] = ones
            return c

        lax.fori_loop(0, 8, turn, 0)

    def scores(t, u, c, mx, qoff=None):
        rows = pl.ds(pl.multiple_of(t * TILE + c * CHUNK, CHUNK), CHUNK)
        left = jnp.concatenate([kbuf[rows, :], kext[rows, :]], axis=1)
        s = jnp.dot(left, qx[u], preferred_element_type=jnp.float32)
        if qoff is not None:
            off = c * CHUNK + lax.broadcasted_iota(jnp.int32, (CHUNK, ROWS), 0)
            s = jnp.where(off <= qoff, s, NEG)
        s_scr[u, c * CHUNK : (c + 1) * CHUNK, :] = s
        part = jnp.max(s.reshape(CHUNK // 8, 8, ROWS), axis=0)
        return part if mx is None else jnp.maximum(mx, part)

    def weigh(u, c, mc):
        s = s_scr[u, c * CHUNK : (c + 1) * CHUNK, :]
        p_scr[u, c * CHUNK : (c + 1) * CHUNK, :] = jnp.exp2(s * SCALE - mc).astype(jnp.bfloat16)

    def row_step(step, carry):
        ph, r = step // 4, step % 4

        @pl.when(ph == 0)
        def _():
            @pl.when((r == 1) | (r == 2))
            def _():
                relay(r + 1)

            receive_row(r)

        for k in range(2):
            q_arrived(ph, 2 * r + k).wait_recv()
        for u in range(UNITS):
            j = 2 * r + u // 2
            qx[u, :DIM, :] = qin[ph, j, :, (u % 2) * DIM : (u % 2 + 1) * DIM].T
            qx[u, DIM:, :] = qfeat[j]

        last = 2 * r + xh
        lanes = z * ROWS + lax.broadcasted_iota(jnp.int32, (1, ROWS), 1)

        mx = None
        for c in range(TILE // CHUNK):
            mx = scores(last, 0, c, mx, lanes)
        top = []
        for u in range(UNITS):
            m = jnp.max(mx, axis=0, keepdims=True)
            mc = m * SCALE
            mx = None
            for c in range(TILE // CHUNK):
                if u < UNITS - 1:
                    mx = scores(last, u + 1, c, mx, lanes + ((u + 1) // 2) * 512)
                else:
                    mx = scores(jnp.maximum(last - 1, 0), 0, c, mx)
                weigh(u, c, mc)
            keys = pl.ds(pl.multiple_of(last * TILE, TILE), TILE)
            acc[u] = jnp.dot(vt[:, keys], p_scr[u], preferred_element_type=jnp.float32)
            top.append(m)

        def back(i, carry):
            tops, mx = carry
            tops = list(tops)
            t = last - 1 - i
            keys = pl.ds(pl.multiple_of(t * TILE, TILE), TILE)
            for u in range(UNITS):
                m = jnp.maximum(tops[u], jnp.max(mx, axis=0, keepdims=True))
                drop = jnp.exp2((tops[u] - m) * SCALE)
                mc = m * SCALE
                mx = None
                for c in range(TILE // CHUNK):
                    if u < UNITS - 1:
                        mx = scores(t, u + 1, c, mx)
                    else:
                        mx = scores(jnp.maximum(t - 1, 0), 0, c, mx)
                    weigh(u, c, mc)
                acc[u] = acc[u] * drop + jnp.dot(
                    vt[:, keys], p_scr[u], preferred_element_type=jnp.float32
                )
                tops[u] = m
            return tuple(tops), mx

        lax.fori_loop(0, jnp.minimum(last, 4), back, (tuple(top), mx))

        for k in range(2):
            j = 2 * r + k
            for n in range(2):
                u = 2 * k + n
                o = acc[u, :DIM, :] * (1.0 / acc[u, DIM : DIM + 1, :])
                obuf[ph, j, :, n * DIM : (n + 1) * DIM] = o.T.astype(jnp.bfloat16)

            @pl.when(j == mine)
            def _():
                local_out(ph).start()

            @pl.when(j != mine)
            def _():
                out_copy(ph, j).start()
        return carry

    def place_out(ph, j):
        return out_hbm.at[:, cols(head(j) * 4 * DIM + ph * 2 * DIM, 2 * DIM)]

    def local_out(ph):
        return pltpu.make_async_copy(obuf.at[ph, mine], place_out(ph, mine), o_send.at[ph, mine])

    def out_copy(ph, j):
        return remote(
            obuf.at[ph, j], place_out(ph, mine), o_send.at[ph, j], o_recv.at[ph, mine], device(j)
        )

    def out_arrived(ph, j):
        return remote(
            obuf.at[ph, j], place_out(ph, j), o_send.at[ph, j], o_recv.at[ph, j], device(j)
        )

    lax.fori_loop(0, 8, row_step, 0)

    for ph in range(2):
        local_out(ph).wait()

    def drain(o, c):
        j = (mine + o) % 8
        for i in range(2):
            kv_copy(i, j).wait_send()
            q_copy(i, j).wait_send()
            out_copy(i, j).wait_send()
            out_arrived(i, j).wait_recv()
        return c

    lax.fori_loop(1, 8, drain, 0)

    def drain_forward(j, c):
        for kind in range(6):
            forward(kind, j, True).wait_send()
        return c

    lax.fori_loop(0, 8, drain_forward, 0)


def on_device(queries, keys, values, doc_lengths):
    bf16, f32 = jnp.bfloat16, jnp.float32
    dma = pltpu.SemaphoreType.DMA
    hbm = pl.BlockSpec(memory_space=pl.ANY)
    return pl.pallas_call(
        kernel,
        out_shape=jax.ShapeDtypeStruct(queries.shape, bf16),
        in_specs=[pl.BlockSpec(memory_space=pltpu.SMEM), hbm, hbm, hbm],
        out_specs=hbm,
        scratch_shapes=[
            pltpu.VMEM((2, 8, ROWS, 2 * DIM), bf16),
            pltpu.VMEM((TOKENS, DIM), bf16),
            pltpu.VMEM((TOKENS, DIM), bf16),
            pltpu.VMEM((VROWS, TOKENS), bf16),
            pltpu.VMEM((TOKENS, DIM), bf16),
            pltpu.VMEM((8, DIM, ROWS), bf16),
            pltpu.VMEM((UNITS, 2 * DIM, ROWS), bf16),
            pltpu.VMEM((UNITS, VROWS, ROWS), f32),
            pltpu.VMEM((UNITS, TILE, ROWS), f32),
            pltpu.VMEM((UNITS, TILE, ROWS), bf16),
            pltpu.VMEM((2, 8, ROWS, 2 * DIM), bf16),
            dma((2, 8)), dma((2, 8)), dma((2, 8)), dma((2, 8)),
            dma((6, 8)), dma((6, 8)), dma((2, 8)), dma((2, 8)),
        ],
        compiler_params=pltpu.CompilerParams(
            collective_id=0, has_side_effects=True, vmem_limit_bytes=48 << 20
        ),
    )(doc_lengths, queries, keys, values)


def solution(mesh):
    placed = (P(("grp", "seq"), None), P(("grp", "seq"), None), P(("grp", "seq"), None), P("grp"))
    return jax.shard_map(
        on_device, mesh=mesh, in_specs=placed, out_specs=P(("grp", "seq"), None), check_vma=False
    )
```

```python
import functools

import jax
import jax.numpy as jnp
from jax import lax
from jax.experimental import pallas as pl
from jax.experimental.pallas import tpu as pltpu
from jax.sharding import PartitionSpec as P

DIM = 128
UNIT = 128
ROWS = 256
TOKENS = 8192
DOCS = 6
TILE = 1024
CHUNK = 512
UNITS = 8
VROWS = 136
SCALE = float(DIM**-0.5 * 1.4426950408889634)
FAR = float(2**21)
NEG = -1e30
MESH = pl.DeviceIdType.MESH


def digits(numbers):
    return sum(n * 4**i for i, n in enumerate(numbers))


ITEMS = (
    ((0, 0), (3, 3), (3, 2), (2, 2), (3, 1), (2, 1), (2, 0), (1, 1), (1, 0)),
    ((1, 1), (1, 0), (0, 0), (3, 3), (3, 2), (3, 1), (2, 2), (2, 1), (2, 0)),
    ((2, 2), (2, 1), (1, 1), (2, 0), (1, 0), (0, 0), (3, 3), (3, 2), (3, 1)),
    ((3, 3), (3, 2), (2, 2), (3, 1), (2, 1), (1, 1), (2, 0), (1, 0), (0, 0)),
)
THIRD, FOURTH = (2, 3, 3, 3), (4, 4, 6, 6)


def by_y(y, values):
    return jnp.where(
        y < 2, jnp.where(y == 0, values[0], values[1]), jnp.where(y == 2, values[2], values[3])
    )


def kernel(
    lengths, q_hbm, k_hbm, v_hbm, out_hbm,
    qin, kbuf, vbuf, vt, kext, qx, acc, m_scr, mx_scr, s_scr, p_scr, obuf,
    q_send, q_recv, a_send, a_recv, f_send, f_recv, o_send, o_recv,
):
    me = lax.axis_index("seq")
    y, x, z = me // 8, (me // 2) % 4, me % 2
    xh, xl = x // 2, x % 2
    mine = 2 * y + xl
    x_mate = y * 8 + (3 - x) * 2 + z
    z_mate = y * 8 + x * 2 + 1 - z
    xz_mate = y * 8 + (3 - x) * 2 + 1 - z

    def device(j):
        return (j // 2) * 8 + (2 * xh + j % 2) * 2 + z

    def head(j):
        return 2 * (j // 2) + (j % 2 + xh) % 2

    def block(j, half, side):
        number = (j // 2) * 8 + (2 * half + j % 2) * 2 + side
        return pl.ds(pl.multiple_of(number * ROWS, ROWS), ROWS)

    def cols(start, size):
        return pl.ds(pl.multiple_of(start, DIM), size)

    def remote(src, dst, send, recv, to):
        return pltpu.make_async_remote_copy(
            src_ref=src, dst_ref=dst, send_sem=send, recv_sem=recv,
            device_id={"seq": to}, device_id_type=MESH,
        )

    def kv_in(which, j_from, j_to):
        hbm, buf = ((k_hbm, kbuf), (v_hbm, vbuf))[which]
        return hbm.at[:, cols(head(j_to) * DIM, DIM)], buf.at[block(j_from, xh, z), :]

    def q_in(j_from, j_to):
        return q_hbm.at[:, cols(head(j_to) * 4 * DIM, 4 * DIM)], qin.at[j_from]

    def kv_copy(which, j_to):
        src, dst = kv_in(which, mine, j_to)
        return remote(src, dst, a_send.at[which, j_to], a_recv.at[which, mine], device(j_to))

    def q_copy(j_to):
        src, dst = q_in(mine, j_to)
        return remote(src, dst, q_send.at[j_to], q_recv.at[mine], device(j_to))

    def kv_arrived(which, j):
        src, dst = kv_in(which, j, mine)
        return remote(src, dst, a_send.at[which, j], a_recv.at[which, j], device(j))

    def q_arrived(j):
        src, dst = q_in(j, mine)
        return remote(src, dst, q_send.at[j], q_recv.at[j], device(j))

    def forward(kind, j, sending):
        buf = (kbuf, vbuf)[kind % 2]
        half, side = xh, z
        if not sending and kind // 2 != 1:
            half = 1 - xh
        if not sending and kind // 2 != 0:
            side = 1 - z
        rows = buf.at[block(j, half, side), :]
        to = (x_mate, z_mate, xz_mate)[kind // 2]
        return remote(rows, rows, f_send.at[kind, j], f_recv.at[kind, j], to)

    barrier = pltpu.get_barrier_semaphore()

    def greet(o, c):
        pl.semaphore_signal(
            barrier, inc=1, device_id={"seq": device((mine + o) % 8)}, device_id_type=MESH
        )
        return c

    lax.fori_loop(1, 8, greet, 0)
    for mate in (x_mate, z_mate, xz_mate):
        pl.semaphore_signal(barrier, inc=1, device_id={"seq": mate}, device_id_type=MESH)
    for which in range(2):
        src, dst = kv_in(which, mine, mine)
        pltpu.make_async_copy(src, dst, a_recv.at[which, mine]).start()
    src, dst = q_in(mine, mine)
    pltpu.make_async_copy(src, dst, q_recv.at[mine]).start()
    pl.semaphore_wait(barrier, 10)

    others = [[2 * ((y + dy) % 4) + (xl + dx) % 2 for dx in range(2)] for dy in range(4)]
    others[0] = others[0][1:]

    def send_kv(dy):
        for j in others[dy]:
            kv_copy(0, j).start()
            kv_copy(1, j).start()

    def send_q(dy):
        for j in others[dy]:
            q_copy(j).start()

    send_kv(0)
    send_kv(1)
    send_kv(2)

    def key_row(i):
        return (y + 4 - i) % 4

    def pass_on(i):
        row = key_row(i)
        for k in range(2):
            j = 2 * row + (xl + k) % 2
            for which in range(2):
                kv_arrived(which, j).wait_recv()
                for mate in (2, 0, 1):
                    forward(2 * mate + which, j, True).start()

    def receive(i):
        row = key_row(i)
        for k in range(2):
            for kind in range(6):
                forward(kind, 2 * row + k, False).wait_recv()

        def turn(n, c):
            rows = pl.ds(pl.multiple_of((8 * row + n) * ROWS, ROWS), ROWS)
            vt[:DIM, rows] = vbuf[rows, :].T
            return c

        lax.fori_loop(0, 8, turn, 0)

    pass_on(0)
    send_q(0)
    send_q(1)
    send_kv(3)

    starts, total = [], jnp.int32(0)
    for d in range(DOCS):
        starts.append(total)
        total = total + lengths[d] * UNIT
    ends = starts[1:] + [total]

    lane = lax.broadcasted_iota(jnp.int32, (1, DIM), 1)
    low, high = jnp.zeros((1, DIM), jnp.int32), jnp.full((1, DIM), TOKENS, jnp.int32)
    for d in range(DOCS):
        low, high = jnp.where(lane == d, starts[d], low), jnp.where(lane == d, ends[d], high)

    def key_features(i, c):
        first = pl.multiple_of(i * ROWS, ROWS)
        token = first + lax.broadcasted_iota(jnp.int32, (ROWS, DIM), 0)
        inside = (token >= low) & (token < high)
        kext[pl.ds(first, ROWS), :] = jnp.where(inside, 0.0, -FAR).astype(jnp.bfloat16)
        return c

    lax.fori_loop(0, TOKENS // ROWS, key_features, 0)
    feature = lax.broadcasted_iota(jnp.int32, (DIM, ROWS), 0)
    low_row, high_row = jnp.full((DIM, ROWS), TOKENS, jnp.int32), jnp.zeros((DIM, ROWS), jnp.int32)
    for d in range(DOCS):
        low_row = jnp.where(feature == d, starts[d], low_row)
        high_row = jnp.where(feature == d, ends[d], high_row)

    def query_features(j, c):
        first = ((j // 2) * 8 + (2 * xh + j % 2) * 2 + z) * ROWS
        token = first + lax.broadcasted_iota(jnp.int32, (DIM, ROWS), 1)
        inside = (token >= low_row) & (token < high_row)
        marks = jnp.where(inside, 1.0, 0.0).astype(jnp.bfloat16)
        for n in range(4):
            qx[j // 2, (j % 2) * 4 + n, DIM:, :] = marks
        return c

    lax.fori_loop(0, 8, query_features, 0)
    first_row = lax.broadcasted_iota(jnp.int32, (VROWS - DIM, TOKENS), 0) == 0
    vt[DIM:, :] = jnp.where(first_row, 1.0, 0.0).astype(jnp.bfloat16)

    pass_on(1)
    pass_on(2)
    send_q(2)
    send_q(3)
    receive(0)

    def scores(r, t, u, c, mx, qoff=None):
        rows = pl.ds(pl.multiple_of(t * TILE + c * CHUNK, CHUNK), CHUNK)
        left = jnp.concatenate([kbuf[rows, :], kext[rows, :]], axis=1)
        s = jnp.dot(left, qx[r, u], preferred_element_type=jnp.float32)
        if qoff is not None:
            off = lax.broadcasted_iota(jnp.int32, (CHUNK, ROWS), 0)
            s = jnp.where(off <= qoff, s, NEG)
        s_scr[u, c * CHUNK : (c + 1) * CHUNK, :] = s
        part = jnp.max(s.reshape(CHUNK // 8, 8, ROWS), axis=0)
        return part if mx is None else jnp.maximum(mx, part)

    def weigh(u, c, mc):
        s = s_scr[u, c * CHUNK : (c + 1) * CHUNK, :]
        p = jnp.exp2(s * SCALE - mc).astype(jnp.bfloat16)
        p_scr[u, c * CHUNK : (c + 1) * CHUNK, :] = p

    lanes = z * ROWS + lax.broadcasted_iota(jnp.int32, (1, ROWS), 1)

    def own_tile(r):
        last = 2 * r + xh
        for k in range(2):
            q_arrived(2 * r + k).wait_recv()
            for n in range(4):
                qx[r, 4 * k + n, :DIM, :] = qin[2 * r + k, :, n * DIM : (n + 1) * DIM].T
        mx = scores(r, last, 0, 0, None, lanes)
        for u in range(UNITS):
            m = jnp.max(mx, axis=0, keepdims=True)
            mc = m * SCALE
            mx = None
            for c in range(TILE // CHUNK):
                if u == UNITS - 1:
                    mx = scores(r, 2 * r, 0, c, mx)
                elif c <= (u + 1) // 4:
                    limit = lanes if c == (u + 1) // 4 else None
                    mx = scores(r, last, u + 1, c, mx, limit)
                if c <= u // 4:
                    weigh(u, c, mc)
            size = (u // 4 + 1) * CHUNK
            keys = pl.ds(pl.multiple_of(last * TILE, TILE), size)
            acc[r, u] = jnp.dot(vt[:, keys], p_scr[u, :size], preferred_element_type=jnp.float32)
            m_scr[r, u : u + 1, :] = m
        mx_scr[...] = mx

    def back(r, t, size, mx=None):
        parts = size // CHUNK
        if mx is None:
            for c in range(parts):
                mx = scores(r, t, 0, c, mx)
        keys = pl.ds(pl.multiple_of(t * TILE, TILE), size)
        for u in range(UNITS):
            old = m_scr[r, u : u + 1, :]
            m = jnp.maximum(old, jnp.max(mx, axis=0, keepdims=True))
            drop = jnp.exp2((old - m) * SCALE)
            mc = m * SCALE
            mx = None
            for c in range(parts):
                weigh(u, c, mc)
                if u < UNITS - 1:
                    mx = scores(r, t, u + 1, c, mx)
            acc[r, u] = acc[r, u] * drop + jnp.dot(
                vt[:, keys], p_scr[u, :size], preferred_element_type=jnp.float32
            )
            m_scr[r, u : u + 1, :] = m

    def place_out(j):
        return out_hbm.at[:, cols(head(j) * 4 * DIM, 4 * DIM)]

    def local_out():
        return pltpu.make_async_copy(obuf.at[mine], place_out(mine), o_send.at[mine])

    def out_copy(j):
        return remote(obuf.at[j], place_out(mine), o_send.at[j], o_recv.at[mine], device(j))

    def out_arrived(j):
        return remote(obuf.at[j], place_out(j), o_send.at[j], o_recv.at[j], device(j))

    def finish(r):
        for k in range(2):
            j = 2 * r + k
            for n in range(4):
                u = 4 * k + n
                o = acc[r, u, :DIM, :] * (1.0 / acc[r, u, DIM : DIM + 1, :])
                obuf[j, :, n * DIM : (n + 1) * DIM] = o.astype(jnp.bfloat16).T

            @pl.when(j == mine)
            def _():
                local_out().start()

            @pl.when(j != mine)
            def _():
                out_copy(j).start()

    def item(step, codes):
        r, kr = codes[0] % 4, codes[1] % 4

        @pl.when(step == 1)
        def _():
            pass_on(3)
            receive(1)

        @pl.when(step == by_y(y, THIRD))
        def _():
            receive(2)

        @pl.when(step == by_y(y, FOURTH))
        def _():
            receive(3)

        @pl.when(r == kr)
        def _():
            own_tile(r)

            @pl.when(xh == 1)
            def _():
                back(r, 2 * r, TILE, mx_scr[...])

        @pl.when((kr == r - 1) | ((kr == r - 2) & (xh == 0)))
        def _():
            back(r, 2 * kr, 2 * TILE)

        @pl.when((kr == r - 2) & (xh == 1))
        def _():
            back(r, 2 * kr + 1, TILE)

        @pl.when(kr == jnp.maximum(r - 2, 0))
        def _():
            finish(r)

        return codes[0] // 4, codes[1] // 4

    rows = by_y(y, [digits([i[0] for i in items]) for items in ITEMS])
    keys = by_y(y, [digits([i[1] for i in items]) for items in ITEMS])
    lax.fori_loop(0, 9, item, (rows, keys))

    local_out().wait()

    def drain(o, c):
        j = (mine + o) % 8
        for which in range(2):
            kv_copy(which, j).wait_send()
        q_copy(j).wait_send()
        out_copy(j).wait_send()
        out_arrived(j).wait_recv()
        return c

    lax.fori_loop(1, 8, drain, 0)

    def drain_forward(j, c):
        for kind in range(6):
            forward(kind, j, True).wait_send()
        return c

    lax.fori_loop(0, 8, drain_forward, 0)


def on_device(queries, keys, values, doc_lengths):
    bf16, f32 = jnp.bfloat16, jnp.float32
    dma = pltpu.SemaphoreType.DMA
    hbm = pl.BlockSpec(memory_space=pltpu.HBM)
    return pl.pallas_call(
        kernel,
        out_shape=jax.ShapeDtypeStruct(queries.shape, bf16),
        in_specs=[pl.BlockSpec(memory_space=pltpu.SMEM), hbm, hbm, hbm],
        out_specs=pl.BlockSpec(memory_space=pl.ANY),
        scratch_shapes=[
            pltpu.VMEM((8, ROWS, 4 * DIM), bf16),
            pltpu.VMEM((TOKENS, DIM), bf16),
            pltpu.VMEM((TOKENS, DIM), bf16),
            pltpu.VMEM((VROWS, TOKENS), bf16),
            pltpu.VMEM((TOKENS, DIM), bf16),
            pltpu.VMEM((4, UNITS, 2 * DIM, ROWS), bf16),
            pltpu.VMEM((4, UNITS, VROWS, ROWS), f32),
            pltpu.VMEM((4, UNITS, ROWS), f32),
            pltpu.VMEM((8, ROWS), f32),
            pltpu.VMEM((UNITS, 2 * TILE, ROWS), f32),
            pltpu.VMEM((UNITS, 2 * TILE, ROWS), bf16),
            pltpu.VMEM((8, ROWS, 4 * DIM), bf16),
            dma((8,)), dma((8,)), dma((2, 8)), dma((2, 8)),
            dma((6, 8)), dma((6, 8)), dma((8,)), dma((8,)),
        ],
        compiler_params=pltpu.CompilerParams(
            collective_id=0, has_side_effects=True, vmem_limit_bytes=67043328
        ),
    )(doc_lengths, queries, keys, values)


def solution(mesh):
    placed = (P(("grp", "seq"), None), P(("grp", "seq"), None), P(("grp", "seq"), None), P("grp"))
    return jax.shard_map(
        on_device, mesh=mesh, in_specs=placed, out_specs=P(("grp", "seq"), None), check_vma=False
    )
```

```python
import functools

import jax
import jax.numpy as jnp
from jax import lax
from jax.experimental import pallas as pl
from jax.experimental.pallas import tpu as pltpu
from jax.sharding import PartitionSpec as P

DIM = 128
UNIT = 128
ROWS = 256
TOKENS = 8192
DOCS = 6
TILE = 1024
CHUNK = 512
UNITS = 8
VROWS = 136
SCALE = float(DIM**-0.5 * 1.4426950408889634)
FAR = float(2**21)
NEG = -1e30
MESH = pl.DeviceIdType.MESH


def digits(numbers):
    return sum(n * 4**i for i, n in enumerate(numbers))


ITEMS = (
    ((0, 0), (1, 1), (1, 0), (2, 2), (2, 1), (2, 0), (3, 3), (3, 2), (3, 1)),
    ((1, 1), (1, 0), (0, 0), (3, 3), (3, 2), (3, 1), (2, 2), (2, 1), (2, 0)),
    ((2, 2), (2, 1), (1, 1), (2, 0), (1, 0), (0, 0), (3, 3), (3, 2), (3, 1)),
    ((3, 3), (3, 2), (2, 2), (3, 1), (2, 1), (1, 1), (2, 0), (1, 0), (0, 0)),
)
THIRD, FOURTH = (3, 3, 3, 3), (6, 4, 6, 6)


def by_y(y, values):
    return jnp.where(
        y < 2, jnp.where(y == 0, values[0], values[1]), jnp.where(y == 2, values[2], values[3])
    )


def kernel(
    lengths, q_hbm, k_hbm, v_hbm, out_hbm,
    qin, kbuf, vbuf, vt, kext, qx, acc, m_scr, mx_scr, s_scr, p_scr, obuf,
    q_send, q_recv, a_send, a_recv, f_send, f_recv, o_send, o_recv,
):
    me = lax.axis_index("seq")
    y, x, z = me // 8, (me // 2) % 4, me % 2
    xh, xl = x // 2, x % 2
    mine = 2 * y + xl
    x_mate = y * 8 + (3 - x) * 2 + z
    z_mate = y * 8 + x * 2 + 1 - z
    xz_mate = y * 8 + (3 - x) * 2 + 1 - z

    def device(j):
        return (j // 2) * 8 + (2 * xh + j % 2) * 2 + z

    def head(j):
        return 2 * (j // 2) + (j % 2 + xh) % 2

    def block(j, half, side):
        number = (j // 2) * 8 + (2 * half + j % 2) * 2 + side
        return pl.ds(pl.multiple_of(number * ROWS, ROWS), ROWS)

    def cols(start, size):
        return pl.ds(pl.multiple_of(start, DIM), size)

    def remote(src, dst, send, recv, to):
        return pltpu.make_async_remote_copy(
            src_ref=src, dst_ref=dst, send_sem=send, recv_sem=recv,
            device_id={"seq": to}, device_id_type=MESH,
        )

    def kv_in(which, j_from, j_to):
        hbm, buf = ((k_hbm, kbuf), (v_hbm, vbuf))[which]
        return hbm.at[:, cols(head(j_to) * DIM, DIM)], buf.at[block(j_from, xh, z), :]

    def q_in(j_from, j_to):
        return q_hbm.at[:, cols(head(j_to) * 4 * DIM, 4 * DIM)], qin.at[j_from]

    def kv_copy(which, j_to):
        src, dst = kv_in(which, mine, j_to)
        return remote(src, dst, a_send.at[which, j_to], a_recv.at[which, mine], device(j_to))

    def q_copy(j_to):
        src, dst = q_in(mine, j_to)
        return remote(src, dst, q_send.at[j_to], q_recv.at[mine], device(j_to))

    def kv_arrived(which, j):
        src, dst = kv_in(which, j, mine)
        return remote(src, dst, a_send.at[which, j], a_recv.at[which, j], device(j))

    def q_arrived(j):
        src, dst = q_in(j, mine)
        return remote(src, dst, q_send.at[j], q_recv.at[j], device(j))

    def forward(kind, j, sending):
        buf = (kbuf, vbuf)[kind % 2]
        half, side = xh, z
        if not sending and kind // 2 != 1:
            half = 1 - xh
        if not sending and kind // 2 != 0:
            side = 1 - z
        rows = buf.at[block(j, half, side), :]
        to = (x_mate, z_mate, xz_mate)[kind // 2]
        return remote(rows, rows, f_send.at[kind, j], f_recv.at[kind, j], to)

    barrier = pltpu.get_barrier_semaphore()

    def greet(o, c):
        pl.semaphore_signal(
            barrier, inc=1, device_id={"seq": device((mine + o) % 8)}, device_id_type=MESH
        )
        return c

    lax.fori_loop(1, 8, greet, 0)
    for mate in (x_mate, z_mate, xz_mate):
        pl.semaphore_signal(barrier, inc=1, device_id={"seq": mate}, device_id_type=MESH)
    for which in range(2):
        src, dst = kv_in(which, mine, mine)
        pltpu.make_async_copy(src, dst, a_recv.at[which, mine]).start()
    src, dst = q_in(mine, mine)
    pltpu.make_async_copy(src, dst, q_recv.at[mine]).start()
    pl.semaphore_wait(barrier, 10)

    far = jnp.where(y == 1, 3, 2)
    steps = (0, 1, far, 5 - far)
    others = [[2 * ((y + dy) % 4) + (xl + dx) % 2 for dx in range(2)] for dy in steps]
    others[0] = others[0][1:]

    def send_kv(dy):
        for j in others[dy]:
            kv_copy(0, j).start()
            kv_copy(1, j).start()

    def send_q(dy):
        for j in others[dy]:
            q_copy(j).start()

    send_kv(0)
    send_kv(1)
    send_kv(2)
    send_kv(3)

    def key_row(i):
        return jnp.where(y == 0, i, (y + 4 - i) % 4)

    def pass_on(i):
        row = key_row(i)
        for k in range(2):
            j = 2 * row + (xl + k) % 2
            for which in range(2):
                kv_arrived(which, j).wait_recv()
                for mate in (2, 0, 1):
                    forward(2 * mate + which, j, True).start()

    def receive(i):
        row = key_row(i)
        for k in range(2):
            for kind in range(6):
                forward(kind, 2 * row + k, False).wait_recv()

        def turn(n, c):
            rows = pl.ds(pl.multiple_of((8 * row + n) * ROWS, ROWS), ROWS)
            vt[:DIM, rows] = vbuf[rows, :].T
            return c

        lax.fori_loop(0, 8, turn, 0)

    pass_on(0)
    send_q(0)
    send_q(1)

    @pl.when(y == 1)
    def _():
        send_q(2)

    starts, total = [], jnp.int32(0)
    for d in range(DOCS):
        starts.append(total)
        total = total + lengths[d] * UNIT
    ends = starts[1:] + [total]

    lane = lax.broadcasted_iota(jnp.int32, (1, DIM), 1)
    low, high = jnp.zeros((1, DIM), jnp.int32), jnp.full((1, DIM), TOKENS, jnp.int32)
    for d in range(DOCS):
        low, high = jnp.where(lane == d, starts[d], low), jnp.where(lane == d, ends[d], high)

    def key_features(i, c):
        first = pl.multiple_of(i * ROWS, ROWS)
        token = first + lax.broadcasted_iota(jnp.int32, (ROWS, DIM), 0)
        inside = (token >= low) & (token < high)
        kext[pl.ds(first, ROWS), :] = jnp.where(inside, 0.0, -FAR).astype(jnp.bfloat16)
        return c

    lax.fori_loop(0, TOKENS // ROWS, key_features, 0)
    feature = lax.broadcasted_iota(jnp.int32, (DIM, ROWS), 0)
    low_row, high_row = jnp.full((DIM, ROWS), TOKENS, jnp.int32), jnp.zeros((DIM, ROWS), jnp.int32)
    for d in range(DOCS):
        low_row = jnp.where(feature == d, starts[d], low_row)
        high_row = jnp.where(feature == d, ends[d], high_row)

    def query_features(j, c):
        first = ((j // 2) * 8 + (2 * xh + j % 2) * 2 + z) * ROWS
        token = first + lax.broadcasted_iota(jnp.int32, (DIM, ROWS), 1)
        inside = (token >= low_row) & (token < high_row)
        marks = jnp.where(inside, 1.0, 0.0).astype(jnp.bfloat16)
        for n in range(4):
            qx[j // 2, (j % 2) * 4 + n, DIM:, :] = marks
        return c

    lax.fori_loop(0, 8, query_features, 0)
    first_row = lax.broadcasted_iota(jnp.int32, (VROWS - DIM, TOKENS), 0) == 0
    vt[DIM:, :] = jnp.where(first_row, 1.0, 0.0).astype(jnp.bfloat16)

    pass_on(1)
    pass_on(2)

    @pl.when(y != 1)
    def _():
        send_q(2)

    send_q(3)
    receive(0)

    def scores(r, t, u, c, mx, qoff=None):
        rows = pl.ds(pl.multiple_of(t * TILE + c * CHUNK, CHUNK), CHUNK)
        left = jnp.concatenate([kbuf[rows, :], kext[rows, :]], axis=1)
        s = jnp.dot(left, qx[r, u], preferred_element_type=jnp.float32)
        if qoff is not None:
            off = lax.broadcasted_iota(jnp.int32, (CHUNK, ROWS), 0)
            s = jnp.where(off <= qoff, s, NEG)
        s_scr[u, c * CHUNK : (c + 1) * CHUNK, :] = s
        part = jnp.max(s.reshape(CHUNK // 8, 8, ROWS), axis=0)
        return part if mx is None else jnp.maximum(mx, part)

    def weigh(u, c, mc):
        s = s_scr[u, c * CHUNK : (c + 1) * CHUNK, :]
        p = jnp.exp2(s * SCALE - mc).astype(jnp.bfloat16)
        p_scr[u, c * CHUNK : (c + 1) * CHUNK, :] = p

    lanes = z * ROWS + lax.broadcasted_iota(jnp.int32, (1, ROWS), 1)

    def own_tile(r):
        last = 2 * r + xh
        for k in range(2):
            q_arrived(2 * r + k).wait_recv()
            for n in range(4):
                qx[r, 4 * k + n, :DIM, :] = qin[2 * r + k, :, n * DIM : (n + 1) * DIM].T
        mx = scores(r, last, 0, 0, None, lanes)
        for u in range(UNITS):
            m = jnp.max(mx, axis=0, keepdims=True)
            mc = m * SCALE
            mx = None
            for c in range(TILE // CHUNK):
                if u == UNITS - 1:
                    mx = scores(r, 2 * r, 0, c, mx)
                elif c <= (u + 1) // 4:
                    limit = lanes if c == (u + 1) // 4 else None
                    mx = scores(r, last, u + 1, c, mx, limit)
                if c <= u // 4:
                    weigh(u, c, mc)
            size = (u // 4 + 1) * CHUNK
            keys = pl.ds(pl.multiple_of(last * TILE, TILE), size)
            acc[r, u] = jnp.dot(vt[:, keys], p_scr[u, :size], preferred_element_type=jnp.float32)
            m_scr[r, u : u + 1, :] = m
        mx_scr[...] = mx

    def back(r, t, size, mx=None):
        parts = size // CHUNK
        if mx is None:
            for c in range(parts):
                mx = scores(r, t, 0, c, mx)
        keys = pl.ds(pl.multiple_of(t * TILE, TILE), size)
        for u in range(UNITS):
            old = m_scr[r, u : u + 1, :]
            m = jnp.maximum(old, jnp.max(mx, axis=0, keepdims=True))
            drop = jnp.exp2((old - m) * SCALE)
            mc = m * SCALE
            mx = None
            for c in range(parts):
                weigh(u, c, mc)
                if u < UNITS - 1:
                    mx = scores(r, t, u + 1, c, mx)
            acc[r, u] = acc[r, u] * drop + jnp.dot(
                vt[:, keys], p_scr[u, :size], preferred_element_type=jnp.float32
            )
            m_scr[r, u : u + 1, :] = m

    def place_out(j):
        return out_hbm.at[:, cols(head(j) * 4 * DIM, 4 * DIM)]

    def local_out():
        return pltpu.make_async_copy(obuf.at[mine], place_out(mine), o_send.at[mine])

    def out_copy(j):
        return remote(obuf.at[j], place_out(mine), o_send.at[j], o_recv.at[mine], device(j))

    def out_arrived(j):
        return remote(obuf.at[j], place_out(j), o_send.at[j], o_recv.at[j], device(j))

    def finish(r):
        for k in range(2):
            j = 2 * r + k
            for n in range(4):
                u = 4 * k + n
                o = acc[r, u, :DIM, :] * (1.0 / acc[r, u, DIM : DIM + 1, :])
                obuf[j, :, n * DIM : (n + 1) * DIM] = o.astype(jnp.bfloat16).T

            @pl.when(j == mine)
            def _():
                local_out().start()

            @pl.when(j != mine)
            def _():
                out_copy(j).start()

    def item(step, codes):
        r, kr = codes[0] % 4, codes[1] % 4

        @pl.when(step == 1)
        def _():
            receive(1)

        @pl.when(step == 2)
        def _():
            pass_on(3)

        @pl.when(step == by_y(y, THIRD))
        def _():
            receive(2)

        @pl.when(step == by_y(y, FOURTH))
        def _():
            receive(3)

        @pl.when(r == kr)
        def _():
            own_tile(r)

            @pl.when(xh == 1)
            def _():
                back(r, 2 * r, TILE, mx_scr[...])

        @pl.when((kr == r - 1) | ((kr == r - 2) & (xh == 0)))
        def _():
            back(r, 2 * kr, 2 * TILE)

        @pl.when((kr == r - 2) & (xh == 1))
        def _():
            back(r, 2 * kr + 1, TILE)

        @pl.when(kr == jnp.maximum(r - 2, 0))
        def _():
            finish(r)

        return codes[0] // 4, codes[1] // 4

    rows = by_y(y, [digits([i[0] for i in items]) for items in ITEMS])
    keys = by_y(y, [digits([i[1] for i in items]) for items in ITEMS])
    lax.fori_loop(0, 9, item, (rows, keys))

    local_out().wait()

    def drain(o, c):
        j = (mine + o) % 8
        for which in range(2):
            kv_copy(which, j).wait_send()
        q_copy(j).wait_send()
        out_copy(j).wait_send()
        out_arrived(j).wait_recv()
        return c

    lax.fori_loop(1, 8, drain, 0)

    def drain_forward(j, c):
        for kind in range(6):
            forward(kind, j, True).wait_send()
        return c

    lax.fori_loop(0, 8, drain_forward, 0)


def on_device(queries, keys, values, doc_lengths):
    bf16, f32 = jnp.bfloat16, jnp.float32
    dma = pltpu.SemaphoreType.DMA
    hbm = pl.BlockSpec(memory_space=pltpu.HBM)
    return pl.pallas_call(
        kernel,
        out_shape=jax.ShapeDtypeStruct(queries.shape, bf16),
        in_specs=[pl.BlockSpec(memory_space=pltpu.SMEM), hbm, hbm, hbm],
        out_specs=pl.BlockSpec(memory_space=pl.ANY),
        scratch_shapes=[
            pltpu.VMEM((8, ROWS, 4 * DIM), bf16),
            pltpu.VMEM((TOKENS, DIM), bf16),
            pltpu.VMEM((TOKENS, DIM), bf16),
            pltpu.VMEM((VROWS, TOKENS), bf16),
            pltpu.VMEM((TOKENS, DIM), bf16),
            pltpu.VMEM((4, UNITS, 2 * DIM, ROWS), bf16),
            pltpu.VMEM((4, UNITS, VROWS, ROWS), f32),
            pltpu.VMEM((4, UNITS, ROWS), f32),
            pltpu.VMEM((8, ROWS), f32),
            pltpu.VMEM((UNITS, 2 * TILE, ROWS), f32),
            pltpu.VMEM((UNITS, 2 * TILE, ROWS), bf16),
            pltpu.VMEM((8, ROWS, 4 * DIM), bf16),
            dma((8,)), dma((8,)), dma((2, 8)), dma((2, 8)),
            dma((6, 8)), dma((6, 8)), dma((8,)), dma((8,)),
        ],
        compiler_params=pltpu.CompilerParams(
            collective_id=0, has_side_effects=True, vmem_limit_bytes=67043328
        ),
    )(doc_lengths, queries, keys, values)


def solution(mesh):
    placed = (P(("grp", "seq"), None), P(("grp", "seq"), None), P(("grp", "seq"), None), P("grp"))
    return jax.shard_map(
        on_device, mesh=mesh, in_specs=placed, out_specs=P(("grp", "seq"), None), check_vma=False
    )
```

```python
import functools

import jax
import jax.numpy as jnp
from jax import lax
from jax.experimental import pallas as pl
from jax.experimental.pallas import tpu as pltpu
from jax.sharding import PartitionSpec as P

DIM = 128
UNIT = 128
ROWS = 256
TOKENS = 8192
DOCS = 6
TILE = 1024
CHUNK = 512
UNITS = 8
VROWS = 136
SCALE = float(DIM**-0.5 * 1.4426950408889634)
FAR = float(2**21)
NEG = -1e30
MESH = pl.DeviceIdType.MESH


def digits(numbers):
    return sum(n * 4**i for i, n in enumerate(numbers))


ITEMS = (
    ((0, 0), (1, 1), (1, 0), (2, 2), (2, 1), (2, 0), (3, 3), (3, 2), (3, 1)),
    ((1, 1), (1, 0), (0, 0), (3, 3), (3, 2), (3, 1), (2, 2), (2, 1), (2, 0)),
    ((2, 2), (2, 1), (1, 1), (2, 0), (1, 0), (0, 0), (3, 3), (3, 2), (3, 1)),
    ((3, 3), (3, 2), (2, 2), (3, 1), (2, 1), (1, 1), (2, 0), (1, 0), (0, 0)),
)
THIRD, FOURTH = (3, 3, 3, 3), (6, 4, 6, 6)


def by_y(y, values):
    return jnp.where(
        y < 2, jnp.where(y == 0, values[0], values[1]), jnp.where(y == 2, values[2], values[3])
    )


def kernel(
    lengths, q_hbm, k_hbm, v_hbm, out_hbm,
    qin, kbuf, vbuf, vt, kext, qx, acc, m_scr, mx_scr, s_scr, p_scr, obuf,
    q_send, q_recv, a_send, a_recv, f_send, f_recv, o_send, o_recv,
):
    me = lax.axis_index("seq")
    y, x, z = me // 8, (me // 2) % 4, me % 2
    xh, xl = x // 2, x % 2
    mine = 2 * y + xl
    x_mate = y * 8 + (3 - x) * 2 + z
    z_mate = y * 8 + x * 2 + 1 - z
    xz_mate = y * 8 + (3 - x) * 2 + 1 - z

    def device(j):
        return (j // 2) * 8 + (2 * xh + j % 2) * 2 + z

    def head(j):
        return 2 * (j // 2) + (j % 2 + xh) % 2

    def block(j, half, side):
        number = (j // 2) * 8 + (2 * half + j % 2) * 2 + side
        return pl.ds(pl.multiple_of(number * ROWS, ROWS), ROWS)

    def cols(start, size):
        return pl.ds(pl.multiple_of(start, DIM), size)

    def remote(src, dst, send, recv, to):
        return pltpu.make_async_remote_copy(
            src_ref=src, dst_ref=dst, send_sem=send, recv_sem=recv,
            device_id={"seq": to}, device_id_type=MESH,
        )

    def kv_in(which, j_from, j_to):
        hbm, buf = ((k_hbm, kbuf), (v_hbm, vbuf))[which]
        return hbm.at[:, cols(head(j_to) * DIM, DIM)], buf.at[block(j_from, xh, z), :]

    def q_in(j_from, j_to):
        return q_hbm.at[:, cols(head(j_to) * 4 * DIM, 4 * DIM)], qin.at[j_from]

    def kv_copy(which, j_to):
        src, dst = kv_in(which, mine, j_to)
        return remote(src, dst, a_send.at[which, j_to], a_recv.at[which, mine], device(j_to))

    def q_copy(j_to):
        src, dst = q_in(mine, j_to)
        return remote(src, dst, q_send.at[j_to], q_recv.at[mine], device(j_to))

    def kv_arrived(which, j):
        src, dst = kv_in(which, j, mine)
        return remote(src, dst, a_send.at[which, j], a_recv.at[which, j], device(j))

    def q_arrived(j):
        src, dst = q_in(j, mine)
        return remote(src, dst, q_send.at[j], q_recv.at[j], device(j))

    def forward(kind, j, sending):
        buf = (kbuf, vbuf)[kind % 2]
        half, side = xh, z
        if not sending and kind // 2 != 1:
            half = 1 - xh
        if not sending and kind // 2 != 0:
            side = 1 - z
        rows = buf.at[block(j, half, side), :]
        to = (x_mate, z_mate, xz_mate)[kind // 2]
        return remote(rows, rows, f_send.at[kind, j], f_recv.at[kind, j], to)

    barrier = pltpu.get_barrier_semaphore()

    def greet(o, c):
        pl.semaphore_signal(
            barrier, inc=1, device_id={"seq": device((mine + o) % 8)}, device_id_type=MESH
        )
        return c

    lax.fori_loop(1, 8, greet, 0)
    for mate in (x_mate, z_mate, xz_mate):
        pl.semaphore_signal(barrier, inc=1, device_id={"seq": mate}, device_id_type=MESH)
    for which in range(2):
        src, dst = kv_in(which, mine, mine)
        pltpu.make_async_copy(src, dst, a_recv.at[which, mine]).start()
    src, dst = q_in(mine, mine)
    pltpu.make_async_copy(src, dst, q_recv.at[mine]).start()
    pl.semaphore_wait(barrier, 10)

    far = jnp.where(y == 1, 3, 2)
    steps = (0, 1, far, 5 - far)
    others = [[2 * ((y + dy) % 4) + (xl + dx) % 2 for dx in range(2)] for dy in steps]
    others[0] = others[0][1:]

    def send_kv(dy):
        for j in others[dy]:
            kv_copy(0, j).start()
            kv_copy(1, j).start()

    def send_q(dy):
        for j in others[dy]:
            q_copy(j).start()

    send_kv(0)
    send_kv(1)
    send_kv(2)
    send_kv(3)

    def key_row(i):
        return jnp.where(y == 0, i, (y + 4 - i) % 4)

    def pass_on(i):
        row = key_row(i)
        for k in range(2):
            j = 2 * row + (xl + k) % 2
            for which in range(2):
                kv_arrived(which, j).wait_recv()
                for mate in (2, 0, 1):
                    forward(2 * mate + which, j, True).start()

    def receive(i):
        row = key_row(i)
        for k in range(2):
            for kind in range(6):
                forward(kind, 2 * row + k, False).wait_recv()

        def turn(n, c):
            rows = pl.ds(pl.multiple_of((8 * row + n) * ROWS, ROWS), ROWS)
            vt[:DIM, rows] = vbuf[rows, :].T
            return c

        lax.fori_loop(0, 8, turn, 0)

    pass_on(0)
    send_q(0)
    send_q(1)

    @pl.when(y == 1)
    def _():
        send_q(2)

    starts, total = [], jnp.int32(0)
    for d in range(DOCS):
        starts.append(total)
        total = total + lengths[d] * UNIT
    ends = starts[1:] + [total]

    lane = lax.broadcasted_iota(jnp.int32, (1, DIM), 1)
    low, high = jnp.zeros((1, DIM), jnp.int32), jnp.full((1, DIM), TOKENS, jnp.int32)
    for d in range(DOCS):
        low, high = jnp.where(lane == d, starts[d], low), jnp.where(lane == d, ends[d], high)

    def key_features(i, c):
        first = pl.multiple_of(i * ROWS, ROWS)
        token = first + lax.broadcasted_iota(jnp.int32, (ROWS, DIM), 0)
        inside = (token >= low) & (token < high)
        kext[pl.ds(first, ROWS), :] = jnp.where(inside, 0.0, -FAR).astype(jnp.bfloat16)
        return c

    lax.fori_loop(0, TOKENS // ROWS, key_features, 0)
    feature = lax.broadcasted_iota(jnp.int32, (DIM, ROWS), 0)
    low_row, high_row = jnp.full((DIM, ROWS), TOKENS, jnp.int32), jnp.zeros((DIM, ROWS), jnp.int32)
    for d in range(DOCS):
        low_row = jnp.where(feature == d, starts[d], low_row)
        high_row = jnp.where(feature == d, ends[d], high_row)

    def query_features(j, c):
        first = ((j // 2) * 8 + (2 * xh + j % 2) * 2 + z) * ROWS
        token = first + lax.broadcasted_iota(jnp.int32, (DIM, ROWS), 1)
        inside = (token >= low_row) & (token < high_row)
        marks = jnp.where(inside, 1.0, 0.0).astype(jnp.bfloat16)
        for n in range(4):
            qx[j // 2, (j % 2) * 4 + n, DIM:, :] = marks
        return c

    lax.fori_loop(0, 8, query_features, 0)
    first_row = lax.broadcasted_iota(jnp.int32, (VROWS - DIM, TOKENS), 0) == 0
    vt[DIM:, :] = jnp.where(first_row, 1.0, 0.0).astype(jnp.bfloat16)

    pass_on(1)
    pass_on(2)

    @pl.when((y == 0) | (y == 3))
    def _():
        send_q(2)

    @pl.when(y != 2)
    def _():
        send_q(3)

    receive(0)

    def scores(r, t, u, c, mx, qoff=None):
        rows = pl.ds(pl.multiple_of(t * TILE + c * CHUNK, CHUNK), CHUNK)
        left = jnp.concatenate([kbuf[rows, :], kext[rows, :]], axis=1)
        s = jnp.dot(left, qx[r, u], preferred_element_type=jnp.float32)
        if qoff is not None:
            off = lax.broadcasted_iota(jnp.int32, (CHUNK, ROWS), 0)
            s = jnp.where(off <= qoff, s, NEG)
        s_scr[u, c * CHUNK : (c + 1) * CHUNK, :] = s
        part = jnp.max(s.reshape(CHUNK // 8, 8, ROWS), axis=0)
        return part if mx is None else jnp.maximum(mx, part)

    def weigh(u, c, mc):
        s = s_scr[u, c * CHUNK : (c + 1) * CHUNK, :]
        p = jnp.exp2(s * SCALE - mc).astype(jnp.bfloat16)
        p_scr[u, c * CHUNK : (c + 1) * CHUNK, :] = p

    lanes = z * ROWS + lax.broadcasted_iota(jnp.int32, (1, ROWS), 1)

    def own_tile(r):
        last = 2 * r + xh
        for k in range(2):
            q_arrived(2 * r + k).wait_recv()
            for n in range(4):
                qx[r, 4 * k + n, :DIM, :] = qin[2 * r + k, :, n * DIM : (n + 1) * DIM].T
        mx = scores(r, last, 0, 0, None, lanes)
        for u in range(UNITS):
            m = jnp.max(mx, axis=0, keepdims=True)
            mc = m * SCALE
            mx = None
            for c in range(TILE // CHUNK):
                if u == UNITS - 1:
                    mx = scores(r, 2 * r, 0, c, mx)
                elif c <= (u + 1) // 4:
                    limit = lanes if c == (u + 1) // 4 else None
                    mx = scores(r, last, u + 1, c, mx, limit)
                if c <= u // 4:
                    weigh(u, c, mc)
            size = (u // 4 + 1) * CHUNK
            keys = pl.ds(pl.multiple_of(last * TILE, TILE), size)
            acc[r, u] = jnp.dot(vt[:, keys], p_scr[u, :size], preferred_element_type=jnp.float32)
            m_scr[r, u : u + 1, :] = m
        mx_scr[...] = mx

    def back(r, t, size, mx=None):
        parts = size // CHUNK
        if mx is None:
            for c in range(parts):
                mx = scores(r, t, 0, c, mx)
        keys = pl.ds(pl.multiple_of(t * TILE, TILE), size)
        for u in range(UNITS):
            old = m_scr[r, u : u + 1, :]
            m = jnp.maximum(old, jnp.max(mx, axis=0, keepdims=True))
            drop = jnp.exp2((old - m) * SCALE)
            mc = m * SCALE
            mx = None
            for c in range(parts):
                weigh(u, c, mc)
                if u < UNITS - 1:
                    mx = scores(r, t, u + 1, c, mx)
            acc[r, u] = acc[r, u] * drop + jnp.dot(
                vt[:, keys], p_scr[u, :size], preferred_element_type=jnp.float32
            )
            m_scr[r, u : u + 1, :] = m

    def place_out(j):
        return out_hbm.at[:, cols(head(j) * 4 * DIM, 4 * DIM)]

    def local_out():
        return pltpu.make_async_copy(obuf.at[mine], place_out(mine), o_send.at[mine])

    def out_copy(j):
        return remote(obuf.at[j], place_out(mine), o_send.at[j], o_recv.at[mine], device(j))

    def out_arrived(j):
        return remote(obuf.at[j], place_out(j), o_send.at[j], o_recv.at[j], device(j))

    def finish(r):
        for k in range(2):
            j = 2 * r + k
            for n in range(4):
                u = 4 * k + n
                o = acc[r, u, :DIM, :] * (1.0 / acc[r, u, DIM : DIM + 1, :])
                obuf[j, :, n * DIM : (n + 1) * DIM] = o.astype(jnp.bfloat16).T

            @pl.when(j == mine)
            def _():
                local_out().start()

            @pl.when(j != mine)
            def _():
                out_copy(j).start()

    def item(step, codes):
        r, kr = codes[0] % 4, codes[1] % 4

        @pl.when(step == 1)
        def _():
            @pl.when(y == 2)
            def _():
                send_q(2)
                send_q(3)

            receive(1)

        @pl.when(step == 2)
        def _():
            pass_on(3)

        @pl.when(step == by_y(y, THIRD))
        def _():
            receive(2)

        @pl.when(step == by_y(y, FOURTH))
        def _():
            receive(3)

        @pl.when(r == kr)
        def _():
            own_tile(r)

            @pl.when(xh == 1)
            def _():
                back(r, 2 * r, TILE, mx_scr[...])

        @pl.when((kr == r - 1) | ((kr == r - 2) & (xh == 0)))
        def _():
            back(r, 2 * kr, 2 * TILE)

        @pl.when((kr == r - 2) & (xh == 1))
        def _():
            back(r, 2 * kr + 1, TILE)

        @pl.when(kr == jnp.maximum(r - 2, 0))
        def _():
            finish(r)

        return codes[0] // 4, codes[1] // 4

    rows = by_y(y, [digits([i[0] for i in items]) for items in ITEMS])
    keys = by_y(y, [digits([i[1] for i in items]) for items in ITEMS])
    lax.fori_loop(0, 9, item, (rows, keys))

    local_out().wait()

    def drain(o, c):
        j = (mine + o) % 8
        for which in range(2):
            kv_copy(which, j).wait_send()
        q_copy(j).wait_send()
        out_copy(j).wait_send()
        out_arrived(j).wait_recv()
        return c

    lax.fori_loop(1, 8, drain, 0)

    def drain_forward(j, c):
        for kind in range(6):
            forward(kind, j, True).wait_send()
        return c

    lax.fori_loop(0, 8, drain_forward, 0)


def on_device(queries, keys, values, doc_lengths):
    bf16, f32 = jnp.bfloat16, jnp.float32
    dma = pltpu.SemaphoreType.DMA
    hbm = pl.BlockSpec(memory_space=pltpu.HBM)
    return pl.pallas_call(
        kernel,
        out_shape=jax.ShapeDtypeStruct(queries.shape, bf16),
        in_specs=[pl.BlockSpec(memory_space=pltpu.SMEM), hbm, hbm, hbm],
        out_specs=pl.BlockSpec(memory_space=pl.ANY),
        scratch_shapes=[
            pltpu.VMEM((8, ROWS, 4 * DIM), bf16),
            pltpu.VMEM((TOKENS, DIM), bf16),
            pltpu.VMEM((TOKENS, DIM), bf16),
            pltpu.VMEM((VROWS, TOKENS), bf16),
            pltpu.VMEM((TOKENS, DIM), bf16),
            pltpu.VMEM((4, UNITS, 2 * DIM, ROWS), bf16),
            pltpu.VMEM((4, UNITS, VROWS, ROWS), f32),
            pltpu.VMEM((4, UNITS, ROWS), f32),
            pltpu.VMEM((8, ROWS), f32),
            pltpu.VMEM((UNITS, 2 * TILE, ROWS), f32),
            pltpu.VMEM((UNITS, 2 * TILE, ROWS), bf16),
            pltpu.VMEM((8, ROWS, 4 * DIM), bf16),
            dma((8,)), dma((8,)), dma((2, 8)), dma((2, 8)),
            dma((6, 8)), dma((6, 8)), dma((8,)), dma((8,)),
        ],
        compiler_params=pltpu.CompilerParams(
            collective_id=0, has_side_effects=True, vmem_limit_bytes=67043328
        ),
    )(doc_lengths, queries, keys, values)


def solution(mesh):
    placed = (P(("grp", "seq"), None), P(("grp", "seq"), None), P(("grp", "seq"), None), P("grp"))
    return jax.shard_map(
        on_device, mesh=mesh, in_specs=placed, out_specs=P(("grp", "seq"), None), check_vma=False
    )
```
